128 devices in a mesh: idx: 8 (over z, y_hi), tp: 16 (over x, y_lo, core).
Axes of the slice: x: 4, y: 4 (y_hi: 2, y_lo: 2; y = y_hi * 2 + y_lo), z: 4, core: 2. Of those that a mesh axis runs over, the one named last changes fastest.
Arguments:
- activations: bfloat16 [8192, 28672], P('idx', 'tp'), may hold values from -6 to 6
- out_grads: bfloat16 [8192, 8192], P('idx', 'tp'), may hold values from -6 to 6
- proj_in: bfloat16 [28672, 64], P('tp'), may hold values from -0.03125 to 0.03125
- proj_out: bfloat16 [8192, 64], P('tp'), may hold values from -0.0625 to 0.0625
- doc_ids: int32 [8192], P('idx'), may hold values from 0 to 1023, never falling along the last dimension, each value on 1 to 32 neighbouring positions
- doc_order: int32 [1024], replicated, may hold values from 0 to 1023, each once
- inv_fisher: float32 [4096, 4096], P('tp'), may hold values from -1 to 3, as said below
- index_grads: bfloat16 [131072, 4096], P(('idx', 'tp')), may hold values from -0.0234375 to 0.0234375
Outputs:
- scores: float32 [1024, 131072], P(None, ('idx', 'tp'))
The draws below stay inside these ranges and needn't reach their ends.
Inputs may be any that keep to these rules, and one draw needn't show every extreme that they name: `inv_fisher`: an estimate of the inverse Fisher of the projected gradients.
All inputs are finite; a program needn't handle non-finite values.
Results may differ from the reference program's by a relative error of at most 0.0029.
Values may be sent and summed in bfloat16 or wider, within the bound.
A program may use at most 128 MiB of HBM per device.

```python
import math
import jax
import jax.numpy as jnp
import numpy as np
from jax import lax

D = 8192
FF = 28672
R = 64
NDOC = 1024
TOKENS = 8192
INDEXED = 131072
KDIM = 4096


def draw_inv_fisher(key, part):
    width = R * R
    first_key, second_key = jax.random.split(jax.random.fold_in(key, 11))
    diagonal = jnp.exp(jax.random.uniform(first_key, (width,), jnp.float32, jnp.log(0.5), jnp.log(2.0)))
    spread = jax.random.normal(second_key, (width, width), jnp.float32)
    spread = spread * (0.5 / jnp.sqrt(jnp.float32(width)))
    return ((spread + spread.T) * 0.70710678 + jnp.diag(diagonal)).astype(jnp.float32)


def shard_levels(key, extent, pieces, smallest, largest):
    level, own = 1.0, jax.random.fold_in(key, 6)
    for dim, parts in pieces:
        draws = jnp.exp(jax.random.uniform(jax.random.fold_in(own, dim), (parts,), jnp.float32, smallest / len(pieces), largest / len(pieces)))
        level = level * jnp.repeat(draws, extent[dim] // parts).reshape([-1 if axis == dim else 1 for axis in range(len(extent))])
    return level


def profile(number_of, total, limit, slope):
    weights = [(1 << 20) // math.isqrt(standing ** slope) + 1 for standing in range(2, number_of + 1)]
    surplus, given = total - limit - (number_of - 1), [1] * (number_of - 1)
    while surplus > 0:
        movable = [i for i in range(number_of - 1) if given[i] < limit]
        whole, budget = sum([weights[i] for i in movable]), surplus
        for i in movable:
            addition = min(limit - given[i], max(1, budget * weights[i] // whole), surplus)
            given[i] = given[i] + addition
            surplus = surplus - addition
    return np.array([limit] + given)


def ragged(key, count, total, most, lean):
    if count == 2:
        one = jax.random.randint(key, (), max(1, total - most), min(most, total - 1) + 1)
        return jnp.stack([one, total - one])
    sizes = jnp.asarray(profile(count, total, most, lean), jnp.int32)
    couples = (count - 1) // 2
    giver, taker = sizes[1:1 + 2 * couples:2], sizes[2:2 + 2 * couples:2]
    margin = jnp.minimum(giver - 1, most - taker)
    moved = jax.random.randint(jax.random.fold_in(key, 1), (couples,), 0, 1 << 20) % (margin + 1)
    sizes = sizes.at[1:1 + 2 * couples:2].set(giver - moved).at[2:2 + 2 * couples:2].set(taker + moved)
    return sizes[jax.random.permutation(jax.random.fold_in(key, 2), count)]


def centred(key, extent, scale, limit, cuts=(), dtype=jnp.bfloat16):
    drawn = jax.random.normal(key, extent, jnp.float32) * scale
    if len(cuts) > 0:
        drawn = shard_levels(key, extent, cuts, -0.22, 0.18) * drawn
    return jnp.clip(drawn, min=-limit, max=limit).astype(dtype)


def setup_inputs(seed: int = 0) -> dict:
    splits = jax.random.split(jax.random.key(seed), 9)
    activations = centred(splits[0], (TOKENS, FF), 1.0, 6.0, ((0, 8), (1, 16)))
    out_grads = centred(splits[1], (TOKENS, D), 1.0, 6.0, ((0, 8), (1, 16)))
    proj_in = centred(splits[2], (FF, R), FF ** -0.5, 0.03125, ((0, 16),))
    proj_out = centred(splits[3], (D, R), D ** -0.5, 0.0625, ((0, 16),))
    doc_ids = jnp.searchsorted(jnp.cumsum(ragged(splits[4], NDOC, TOKENS, 4 * TOKENS // NDOC, 1)), jnp.arange(TOKENS), side="right").astype(jnp.int32)
    doc_order = jax.random.permutation(splits[5], NDOC).astype(jnp.int32)
    inv_fisher = draw_inv_fisher(jax.random.fold_in(splits[8], 71), 0)
    index_grads = centred(splits[7], (INDEXED, KDIM), (16 * R * R) ** -0.5, 0.0234375, ((0, 128),))
    return dict(activations=activations, out_grads=out_grads, proj_in=proj_in, proj_out=proj_out, doc_ids=doc_ids, doc_order=doc_order, inv_fisher=inv_fisher, index_grads=index_grads)


def reference(activations, out_grads, proj_in, proj_out, doc_ids, doc_order, inv_fisher, index_grads):
    proj_acts = jnp.dot(activations, proj_in, preferred_element_type=jnp.float32)
    proj_grads = jnp.dot(out_grads, proj_out, preferred_element_type=jnp.float32)
    token_grads = (proj_grads[:, :, None] * proj_acts[:, None, :]).reshape(TOKENS, R * R)
    membership = (doc_ids[:, None] == doc_order[None, :]).astype(jnp.float32)
    doc_grads = lax.dot_general(membership, token_grads, (((0,), (0,)), ((), ())),
                                precision=lax.Precision.HIGHEST, preferred_element_type=jnp.float32)
    conditioned = jnp.dot(doc_grads, inv_fisher, precision=lax.Precision.HIGHEST,
                          preferred_element_type=jnp.float32)
    queries = conditioned.astype(jnp.bfloat16)
    return lax.dot_general(queries, index_grads, (((1,), (1,)), ((), ())),
                           preferred_element_type=jnp.float32)
```

```python
import functools

import jax
import jax.numpy as jnp
from jax import lax
from jax.experimental import pallas as pl
from jax.experimental.pallas import tpu as pltpu
from jax.sharding import PartitionSpec as P

MESH = pl.DeviceIdType.MESH
F32, BF16 = jnp.float32, jnp.bfloat16
AXES = "xyz"
LINKS = (("x", 0), ("y", 0), ("z", 0), ("x", 1), ("y", 1), ("z", 1))
COLOURS = 6
MESSAGES = [(s, b) for s in range(1, 7) for b in range(s)]
SLOT = {m: i for i, m in enumerate(MESSAGES)}
PASSES = 12


class Place:
    def __init__(self):
        idx, tp = lax.axis_index("idx"), lax.axis_index("tp")
        self.x, self.z = tp // 4, idx // 2
        self.y = lax.rem(idx, 2) * 2 + lax.rem(tp // 2, 2)
        self.core = lax.rem(tp, 2)

    def device(self, x=None, y=None, z=None, core=None):
        x = self.x if x is None else x
        y = self.y if y is None else y
        z = self.z if z is None else z
        core = self.core if core is None else core
        return (z * 2 + y // 2, (x * 2 + lax.rem(y, 2)) * 2 + core)

    def across(self, axis, kind):
        v = getattr(self, axis)
        if kind:
            return lax.rem(v + 3 + 2 * lax.rem(v, 2), 4)
        return v + 1 - 2 * lax.rem(v, 2)

    def mate(self):
        return self.device(core=1 - self.core)

    def next_to(self, axis, kind):
        return self.device(**{axis: self.across(axis, kind)})


def order_of(colour):
    return [LINKS[(colour + s) % 6] for s in range(6)]


def turned(colour, axis):
    order = order_of(colour)
    return 1 if order.index((axis, 1)) < order.index((axis, 0)) else 0


def spot(v, turn):
    return lax.rem(v + 3 * turn, 4)


def boxes_at(colour, where):
    own = {a: spot(where[a], turned(colour, a)) for a in AXES}
    seen = dict.fromkeys(AXES, 0)

    def held(a):
        p = own[a]
        return ((p, 1), (p - lax.rem(p, 2), 2), (0, 4))[seen[a]]

    boxes = [{a: held(a) for a in AXES}]
    for axis, _ in order_of(colour):
        box = {a: held(a) for a in AXES}
        p = own[axis]
        box[axis] = (2 * (1 - p // 2), 2) if seen[axis] else (p + 1 - 2 * lax.rem(p, 2), 1)
        boxes.append(box)
        seen[axis] += 1
    return boxes


def part_of(buf, core, box):
    return buf.at[core, pl.ds(*box["z"]), pl.ds(*box["y"]), pl.ds(*box["x"])]


class Gather:
    def __init__(self, me, bufs, sems):
        self.me, self.bufs = me, bufs
        self.out_sem, self.in_sem, self.pass_out, self.pass_in = sems
        here = {a: getattr(me, a) for a in AXES}
        self.boxes = [boxes_at(k, here) for k in range(COLOURS)]
        self.theirs = []
        for k in range(COLOURS):
            per_step = []
            for axis, kind in order_of(k):
                per_step.append(boxes_at(k, {**here, axis: me.across(axis, kind)}))
            self.theirs.append(per_step)

    @staticmethod
    def semaphores():
        dma = pltpu.SemaphoreType.DMA
        return [dma((COLOURS, 21)), dma((COLOURS, 21)), dma((COLOURS, PASSES)), dma((COLOURS, PASSES))]

    def message(self, k, s, b):
        ref = part_of(self.bufs[k], self.me.core, self.boxes[k][b])
        axis, kind = order_of(k)[s - 1]
        return pltpu.make_async_remote_copy(
            src_ref=ref, dst_ref=ref,
            send_sem=self.out_sem.at[k, SLOT[s, b]], recv_sem=self.in_sem.at[k, SLOT[s, b]],
            device_id=self.me.next_to(axis, kind), device_id_type=MESH)

    def arrival(self, k, s, b):
        ref = part_of(self.bufs[k], self.me.core, self.theirs[k][s - 1][b])
        axis, kind = order_of(k)[s - 1]
        return pltpu.make_async_remote_copy(
            src_ref=ref, dst_ref=ref,
            send_sem=self.out_sem.at[k, SLOT[s, b]], recv_sem=self.in_sem.at[k, SLOT[s, b]],
            device_id=self.me.next_to(axis, kind), device_id_type=MESH)

    def pass_box(self, k, n):
        return self.boxes[k][n] if n < 6 else self.theirs[k][5][n - 6]

    def passed(self, k, n, core):
        ref = part_of(self.bufs[k], core, self.pass_box(k, n))
        return pltpu.make_async_remote_copy(
            src_ref=ref, dst_ref=ref,
            send_sem=self.pass_out.at[k, n], recv_sem=self.pass_in.at[k, n],
            device_id=self.me.mate(), device_id_type=MESH)

    def start(self):
        for s in range(1, 7):
            for k in range(COLOURS):
                self.message(k, s, 0).start()
            if s == 1:
                for k in range(COLOURS):
                    self.passed(k, 0, self.me.core).start()

    def step(self, s):
        for k in range(COLOURS):
            for b in range(s):
                self.arrival(k, s, b).wait_recv()
            for later in range(s + 1, 7):
                self.message(k, later, s).start()
            self.passed(k, s, self.me.core).start()

    def last(self, b):
        for k in range(COLOURS):
            self.arrival(k, 6, b).wait_recv()
            self.passed(k, 6 + b, self.me.core).start()

    def from_mate(self, n):
        for k in range(COLOURS):
            self.passed(k, n, 1 - self.me.core).wait_recv()

    def close(self):
        for k in range(COLOURS):
            for s, b in MESSAGES:
                self.message(k, s, b).wait_send()
            for n in range(PASSES):
                self.passed(k, n, self.me.core).wait_send()


def greet(devices):
    barrier = pltpu.get_barrier_semaphore()
    for device in devices:
        pl.semaphore_signal(barrier, inc=1, device_id=device, device_id_type=MESH)
    pl.semaphore_wait(barrier, len(devices))


Q_TILES = (3, 3, 3, 3, 2, 2)
Q_FIRST = (0, 3, 6, 9, 12, 14)


def scores_kernel(blk_ref, g_hbm, out_ref, b0, b1, b2, b3, b4, b5, g_ref, g_sem, *sems):
    me = Place()
    bufs = (b0, b1, b2, b3, b4, b5)
    load = pltpu.make_async_copy(g_hbm, g_ref, g_sem)
    load.start()
    gather = Gather(me, bufs, sems)
    for k in range(COLOURS):
        own = gather.boxes[k][0]
        bufs[k][me.core, own["z"][0], own["y"][0], own["x"][0]] = blk_ref[Q_FIRST[k]:Q_FIRST[k] + Q_TILES[k]]
    greet([me.next_to(a, t) for a, t in LINKS] + [me.mate()])
    gather.start()
    for s in range(1, 6):
        gather.step(s)
    for b in range(6):
        gather.last(b)
    for n in range(PASSES):
        gather.from_mate(n)
    load.wait()

    @pl.loop(0, 8)
    def _(chunk):
        z_low, y = chunk // 4, lax.rem(chunk, 4)
        depth = pl.multiple_of(chunk * 512, 512)
        g = g_ref[:, pl.ds(depth, 512)]
        for z_high in range(2):
            for core in range(2):
                cols = []
                for x in range(4):
                    rows = []
                    for k in range(COLOURS):
                        tile = bufs[k][core, spot(z_high * 2 + z_low, turned(k, "z")),
                                       spot(y, turned(k, "y")), (x + 3 * turned(k, "x")) % 4]
                        rows.append(tile.reshape(Q_TILES[k] * 16, 128))
                    cols.append(jnp.concatenate(rows, 0))
                lhs = jnp.concatenate(cols, 1)
                got = lax.dot_general(lhs, g, (((1,), (1,)), ((), ())), preferred_element_type=F32)
                rows = pl.ds((core * 2 + z_high) * 256, 256)

                @pl.when(chunk == 0)
                def _():
                    out_ref[rows, :] = got

                @pl.when(chunk > 0)
                def _():
                    out_ref[rows, :] += got

    gather.close()


def scores_call(block, index_grads):
    vmem = pl.BlockSpec(memory_space=pltpu.VMEM)
    return pl.pallas_call(
        scores_kernel,
        out_shape=jax.ShapeDtypeStruct((1024, 1024), F32),
        in_specs=[vmem, pl.BlockSpec(memory_space=pl.ANY)],
        out_specs=vmem,
        scratch_shapes=[pltpu.VMEM((2, 4, 4, 4, n, 16, 128), BF16) for n in Q_TILES]
        + [pltpu.VMEM((1024, 4096), BF16), pltpu.SemaphoreType.DMA] + Gather.semaphores(),
        compiler_params=pltpu.CompilerParams(collective_id=3, has_side_effects=True, vmem_limit_bytes=48 << 20),
        name="scores",
    )(block, index_grads)


T_UNITS = (3, 3, 3, 3, 2, 2)
T_FIRST = (0, 3, 6, 9, 12, 14)
OTHERS_TP = [(dx, dy) for dx in range(4) for dy in range(2)][1:]
OTHERS_IDX = [(dz, dy) for dz in range(4) for dy in range(2)][1:]
PITCH = 264


def halves(v):
    high = v.astype(BF16)
    return high, (v - high.astype(F32)).astype(BF16)


def queries_kernel(
    part_ref, f_hbm, counts_ref, out_ref,
    from_mate, mine, arrived, t0, t1, t2, t3, t4, t5, tok, fisher, their_counts, counts_sum, counts, dg, acc, lacc,
    mate_sem, rs_out, rs_in, f_out, f_in, f_pass, f_own, c_out, c_in, c_sem, *sems):
    me = Place()
    bufs = (t0, t1, t2, t3, t4, t5)
    low = lax.rem(me.y, 2)
    high = me.y // 2
    p = low * 4 + me.x
    core = me.core

    def tp_mate(dx, dy):
        return lax.rem(me.x + dx, 4), lax.rem(low + dy, 2)

    def idx_mate(dz, dy):
        return me.device(z=lax.rem(me.z + dz, 4), y=lax.rem(high + dy, 2) * 2 + low)

    others = [me.device(x=x, y=high * 2 + y) for x, y in (tp_mate(*d) for d in OTHERS_TP)]
    far = [idx_mate(*d) for d in OTHERS_IDX]
    greet([me.next_to(a, t) for a, t in LINKS] + [me.mate()] + others + far)

    def remote(src, dst, s, r, device):
        return pltpu.make_async_remote_copy(src_ref=src, dst_ref=dst, send_sem=s, recv_sem=r,
                                            device_id=device, device_id_type=MESH)

    to_mate = remote(part_ref.at[:, 1 - core], from_mate, mate_sem.at[0], mate_sem.at[1], me.mate())
    to_mate.start()
    shard = lax.axis_index("idx")
    count_copies = []
    for n, device in enumerate(far):
        copy = remote(counts_ref, their_counts.at[shard], c_out.at[n], c_in.at[n], device)
        copy.start()
        count_copies.append(copy)

    def columns(x, y_low):
        block = lax.rem(me.z, 2) * 16 + (high * 2 + y_low) * 4 + x
        return f_hbm.at[:, pl.ds(pl.multiple_of(block * 128, 128), 128)]

    place = me.x * 2 + low
    f_copies = []
    for n, d in enumerate(OTHERS_TP):
        f_copies.append(remote(columns(*tp_mate(*d)), fisher.at[place, core], f_out.at[n], f_in.at[n], others[n]))
    own_f = pltpu.make_async_copy(columns(me.x, low), fisher.at[place, core], f_own)
    own_f.start()

    to_mate.wait()
    for q in range(8):
        mine[q] = part_ref[q, core] + from_mate[q]
    arrived[p] = mine[p]
    rs_copies = []
    for n, d in enumerate(OTHERS_TP):
        x, y = tp_mate(*d)
        copy = remote(mine.at[y * 4 + x], arrived.at[p], rs_out.at[n], rs_in.at[n], others[n])
        copy.start()
        rs_copies.append(copy)
    for copy in f_copies:
        copy.start()
    for copy in rs_copies:
        copy.wait_recv()
    total = arrived[0]
    for q in range(1, 8):
        total = total + arrived[q]
    gather = Gather(me, bufs, sems)
    for k in range(COLOURS):
        own = gather.boxes[k][0]
        for u in range(T_UNITS[k]):
            row = (T_FIRST[k] + u) * 4
            bufs[k][core, own["z"][0], own["y"][0], own["x"][0], u] = total[row:row + 4]
    gather.start()

    their_counts[shard] = counts_ref[...]
    for copy in count_copies:
        copy.wait_recv()
    summed = their_counts[0]
    for n in range(1, 8):
        summed = summed + their_counts[n]
    counts_sum[...] = summed
    to_scalar = pltpu.make_async_copy(counts_sum, counts, c_sem)
    to_scalar.start()
    to_scalar.wait()

    for s in range(1, 6):
        gather.step(s)
        if s == 4:
            own_f.wait()
            for copy in f_copies:
                copy.wait_recv()
            pass_f = remote(fisher.at[:, core], fisher.at[:, core], f_pass.at[0], f_pass.at[1], me.mate())
            pass_f.start()
    for b in range(6):
        gather.last(b)
    for n in range(PASSES):
        gather.from_mate(n)

    @pl.loop(0, 64)
    def _(chip):
        z, y, x = chip // 16, lax.rem(chip // 4, 4), lax.rem(chip, 4)
        for c in range(2):
            base = pl.multiple_of(chip * 128 + c * 64, 64)
            for k in range(COLOURS):
                for u in range(T_UNITS[k]):
                    tok[pl.ds(base + (T_FIRST[k] + u) * 4, 4), :] = bufs[k][
                        c, spot(z, turned(k, "z")), spot(y, turned(k, "y")), spot(x, turned(k, "x")), u]

    tok[8192:8224, :] = jnp.zeros((32, 128), F32)

    first_row = (core * 2 + me.z // 2) * 256
    lane = lax.broadcasted_iota(jnp.int32, (128, 128), 1)
    sub = lax.broadcasted_iota(jnp.int32, (32, 128), 0)
    same = lax.broadcasted_iota(jnp.int32, (128, 256), 0) // 32 == lax.rem(
        lax.broadcasted_iota(jnp.int32, (128, 256), 1), 128) // 32

    @pl.loop(0, 64)
    def _(group):
        rows = []
        for q in range(4):
            r = first_row + group * 4 + q
            start = counts[r // 128, lax.rem(r, 128)]
            length = counts[8 + r // 128, lax.rem(r, 128)]
            rows.append(jnp.where(sub < length, tok[pl.ds(start, 32), :], 0.0))
        pieces = jnp.concatenate(rows, 0)
        turned_pieces = pieces.T
        lead = jnp.concatenate([turned_pieces[64:96], turned_pieces[96:128]], 1)
        lead = jnp.where(same, jnp.concatenate([lead] * 4, 0), 0.0)
        lead_high, lead_low = halves(lead)
        top = jnp.where(lane < 64, pieces, 0.0)
        bottom = jnp.where(lane < 64, 0.0, pltpu.roll(pieces, 64, 1))
        right_high, right_low = halves(jnp.concatenate([top, bottom], 0))
        both = jnp.dot(lead_high, jnp.concatenate([right_high, right_low], 1), preferred_element_type=F32)
        rest = jnp.dot(lead_low, right_high, preferred_element_type=F32)
        got = both[:, :128] + both[:, 128:] + rest
        for q in range(4):
            dg[pl.ds(group * 4 + q, 32, stride=PITCH), :] = got[q * 32:(q + 1) * 32]

    pass_f.wait_recv()
    acc[...] = jnp.zeros_like(acc)
    lacc[...] = jnp.zeros_like(lacc)

    @pl.loop(0, 16)
    def _(kk):
        left = dg[pl.ds(pl.multiple_of(kk * 2 * PITCH, 8), 256), :]
        right = dg[pl.ds(pl.multiple_of((kk * 2 + 1) * PITCH, 8), 256), :]
        d_high, d_low = halves(jnp.concatenate([left, right], 1))
        f_high, f_low = halves(fisher[kk // 2, lax.rem(kk, 2)])
        acc[...] += jnp.dot(d_high, jnp.concatenate([f_high, f_low], 1), preferred_element_type=F32)
        lacc[...] += jnp.dot(d_low, f_high, preferred_element_type=F32)

    result = acc[:, :128] + acc[:, 128:] + lacc[...]
    out_ref[...] = result.astype(BF16).reshape(16, 16, 128)

    for copy in count_copies + f_copies + rs_copies + [pass_f]:
        copy.wait_send()
    gather.close()


def queries_call(part, inv_fisher, counts):
    vmem = pl.BlockSpec(memory_space=pltpu.VMEM)
    dma = pltpu.SemaphoreType.DMA
    return pl.pallas_call(
        queries_kernel,
        out_shape=jax.ShapeDtypeStruct((16, 16, 128), BF16),
        in_specs=[vmem, pl.BlockSpec(memory_space=pl.ANY), vmem],
        out_specs=vmem,
        scratch_shapes=[
            pltpu.VMEM((8, 64, 128), F32), pltpu.VMEM((8, 64, 128), F32), pltpu.VMEM((8, 64, 128), F32)]
        + [pltpu.VMEM((2, 4, 4, 4, n, 4, 128), F32) for n in T_UNITS]
        + [pltpu.VMEM((8224, 128), F32), pltpu.VMEM((8, 2, 256, 128), F32),
           pltpu.VMEM((8, 16, 128), jnp.int32), pltpu.VMEM((16, 128), jnp.int32), pltpu.SMEM((16, 128), jnp.int32),
           pltpu.VMEM((32 * PITCH, 128), F32), pltpu.VMEM((256, 256), F32), pltpu.VMEM((256, 128), F32),
           dma((2,)), dma((7,)), dma((7,)), dma((7,)), dma((7,)), dma((2,)), dma, dma((7,)), dma((7,)), dma]
        + Gather.semaphores(),
        compiler_params=pltpu.CompilerParams(collective_id=2, has_side_effects=True, vmem_limit_bytes=48 << 20),
        name="queries",
    )(part, inv_fisher, counts)


def per_device(activations, out_grads, proj_in, proj_out, doc_ids, doc_order, inv_fisher, index_grads):
    lead_pairs = proj_out.reshape(-1, 32, 2).transpose(0, 2, 1).reshape(-1, 64)
    part = jnp.concatenate([
        jnp.dot(activations, proj_in, preferred_element_type=F32),
        jnp.dot(out_grads, lead_pairs, preferred_element_type=F32)], 1)
    before = jnp.sum((doc_ids[:, None] < doc_order[None, :]).astype(jnp.int32), 0)
    equal = jnp.sum((doc_ids[:, None] == doc_order[None, :]).astype(jnp.int32), 0)
    counts = jnp.concatenate([before.reshape(8, 128), equal.reshape(8, 128)], 0)
    block = queries_call(part.reshape(8, 2, 64, 128), inv_fisher, counts)
    return scores_call(block, index_grads)


def solution(mesh):
    placed = (
        P("idx", "tp"), P("idx", "tp"), P("tp", None), P("tp", None),
        P("idx"), P(), P("tp", None), P(("idx", "tp"), None),
    )
    return jax.shard_map(
        per_device, mesh=mesh, in_specs=placed, out_specs=P(None, ("idx", "tp")), check_vma=False)
```

```python
import functools

import jax
import jax.numpy as jnp
from jax import lax
from jax.experimental import pallas as pl
from jax.experimental.pallas import tpu as pltpu
from jax.sharding import PartitionSpec as P

MESH = pl.DeviceIdType.MESH
F32, BF16 = jnp.float32, jnp.bfloat16
LINKS = (("x", 0), ("y", 0), ("z", 0), ("x", 1), ("y", 1), ("z", 1))
COLOURS = 6


class Place:
    def __init__(self):
        idx, tp = lax.axis_index("idx"), lax.axis_index("tp")
        self.x, self.z = tp // 4, idx // 2
        self.y = lax.rem(idx, 2) * 2 + lax.rem(tp // 2, 2)
        self.core = lax.rem(tp, 2)

    def device(self, x=None, y=None, z=None, core=None):
        x = self.x if x is None else x
        y = self.y if y is None else y
        z = self.z if z is None else z
        core = self.core if core is None else core
        return (z * 2 + y // 2, (x * 2 + lax.rem(y, 2)) * 2 + core)

    def across(self, axis, kind):
        v = getattr(self, axis)
        if kind:
            return lax.rem(v + 3 + 2 * lax.rem(v, 2), 4)
        return v + 1 - 2 * lax.rem(v, 2)

    def mate(self):
        return self.device(core=1 - self.core)

    def next_to(self, axis, kind):
        return self.device(**{axis: self.across(axis, kind)})


SUBSETS = [tuple(s for s in (0, 1, 2) if n >> s & 1) for n in (0, 1, 2, 4, 3, 5, 6, 7)]
OCTETS = [(), (3,), (4,), (3, 4), (5,), (3, 5), (4, 5), (3, 4, 5)]


def order_of(colour):
    return [LINKS[(colour + s) % 6] for s in range(6)]


def turned(colour, axis):
    order = order_of(colour)
    return 1 if order.index((axis, 1)) < order.index((axis, 0)) else 0


def spot(v, turn):
    return lax.rem(v + 3 * turn, 4)


class Gather:
    def __init__(self, me, bufs, sems):
        self.me, self.bufs = me, bufs
        self.out_sem, self.in_sem, self.pass_out, self.pass_in = sems
        self.places = {}
        for axis in "xyz":
            for turn in range(2):
                p = spot(getattr(me, axis), turn)
                over = lax.rem(p + 3 + 2 * lax.rem(p, 2), 4)
                for crossed, base in enumerate((p, over)):
                    self.places[axis, turn, 0, crossed] = base
                    self.places[axis, turn, 1, crossed] = base + 1 - 2 * lax.rem(base, 2)

    @staticmethod
    def semaphores():
        dma = pltpu.SemaphoreType.DMA
        return [dma((COLOURS, 15)), dma((COLOURS, 16)), dma((COLOURS, 8)), dma((COLOURS, 8))]

    def at(self, k, subset, octet):
        order = order_of(k)
        got = []
        for axis in "zyx":
            flip = any(order[s][0] == axis for s in subset)
            crossed = any(order[s][0] == axis for s in octet)
            got.append(self.places[axis, turned(k, axis), int(flip), int(crossed)])
        return got

    def cell(self, k, octet):
        got = []
        for axis in "zyx":
            crossed = any(order_of(k)[s][0] == axis for s in octet)
            base = self.places[axis, turned(k, axis), 0, int(crossed)]
            got.append(base - lax.rem(base, 2))
        return got

    def cell_ref(self, k, core, octet):
        z, y, x = self.cell(k, octet)
        return self.bufs[k].at[core, pl.ds(z, 2), pl.ds(y, 2), pl.ds(x, 2)]

    def send(self, k, ref, out, into, device):
        return pltpu.make_async_remote_copy(
            src_ref=ref, dst_ref=ref, send_sem=self.out_sem.at[k, out], recv_sem=self.in_sem.at[k, into],
            device_id=device, device_id_type=MESH)

    def direct(self, k, n):
        move = {}
        for s in SUBSETS[n]:
            axis, kind = order_of(k)[s]
            move[axis] = self.me.across(axis, kind)
        ref = self.bufs[k].at[(self.me.core, *self.at(k, (), ()))]
        return self.send(k, ref, n, n, self.me.device(**move))

    def onward(self, k, step, octet):
        axis, kind = order_of(k)[step]
        reached = OCTETS.index(octet + (step,))
        return self.send(k, self.cell_ref(k, self.me.core, octet), 7 + reached, 8 + reached,
                         self.me.next_to(axis, kind))

    def arrive(self, k, octet):
        if octet:
            ref = self.cell_ref(k, self.me.core, octet)
            self.send(k, ref, 0, 8 + OCTETS.index(octet), self.me.mate()).wait_recv()
            return
        for n in range(1, 8):
            ref = self.bufs[k].at[(self.me.core, *self.at(k, SUBSETS[n], ()))]
            self.send(k, ref, 0, n, self.me.mate()).wait_recv()

    def passed(self, k, octet, core):
        n = OCTETS.index(octet)
        ref = self.cell_ref(k, core, octet)
        return pltpu.make_async_remote_copy(
            src_ref=ref, dst_ref=ref, send_sem=self.pass_out.at[k, n], recv_sem=self.pass_in.at[k, n],
            device_id=self.me.mate(), device_id_type=MESH)

    def start(self):
        for n in range(1, 8):
            for k in range(COLOURS):
                self.direct(k, n).start()

    def forward(self, step, octet):
        for k in range(COLOURS):
            self.onward(k, step, octet).start()

    def take(self, octet):
        step = max((2,) + octet) + 1
        for k in range(COLOURS):
            self.arrive(k, octet)
            if step < 6:
                self.onward(k, step, octet).start()
        if octet == ():
            self.forward(4, ())
        if octet == (3,):
            self.forward(5, ())
            self.forward(5, (3,))
        for k in range(COLOURS):
            self.passed(k, octet, self.me.core).start()

    def from_mate(self, octet):
        for k in range(COLOURS):
            self.passed(k, octet, 1 - self.me.core).wait_recv()

    def close(self):
        for k in range(COLOURS):
            for n in range(1, 8):
                self.direct(k, n).wait_send()
            for octet in OCTETS:
                for step in range(max((2,) + octet) + 1, 6):
                    self.onward(k, step, octet).wait_send()
                self.passed(k, octet, self.me.core).wait_send()


def cell_mates(me):
    found = {}
    for k in range(COLOURS):
        for subset in SUBSETS[1:]:
            steps = tuple(sorted(order_of(k)[n] for n in subset))
            found[steps] = me.device(**{axis: me.across(axis, kind) for axis, kind in steps})
    return list(found.values()) + [me.mate()]


def remote(src, dst, s, r, device):
    return pltpu.make_async_remote_copy(
        src_ref=src, dst_ref=dst, send_sem=s, recv_sem=r, device_id=device, device_id_type=MESH)


def halves(v):
    high = v.astype(BF16)
    return high, (v - high.astype(F32)).astype(BF16)


UNITS = (3, 3, 3, 3, 2, 2)
FIRST = (0, 3, 6, 9, 12, 14)
T_UNITS = (2, 1, 1, 2, 1, 1)
T_FIRST = (0, 2, 3, 4, 6, 7)
OTHERS_TP = [(dx, dy) for dx in range(4) for dy in range(2)][1:]
OTHERS_IDX = [(dz, dy) for dz in range(4) for dy in range(2)][1:]
PITCH = 264
LANES = (((1,), (1,)), ((), ()))


def multiply(gather, k, crossed, bufs, gt_ref, out_ref):
    rows = UNITS[k] * 16
    lows = {}
    for step, over in crossed.items():
        axis = order_of(k)[step][0]
        low = gather.places[axis, turned(k, axis), 0, over]
        lows[axis] = low - lax.rem(low, 2)

    def spots_of(axis):
        return [lows[axis] + n for n in range(2)] if axis in lows else list(range(4))

    def natural(p, a):
        return lax.rem(p + turned(k, a), 4)

    def product(spots, out_rows):
        starts = []
        for _, z, y, x in spots[0]:
            zn, yn, xn = natural(z, "z"), natural(y, "y"), natural(x, "x")
            starts.append(pl.multiple_of((lax.rem(zn, 2) * 16 + yn * 4 + xn) * 128, 128))
        lhs = jnp.concatenate([
            jnp.concatenate([bufs[k][s].reshape(rows, 128) for s in blocks], 1) for blocks in spots], 0)
        for tile in range(4):
            cols = pl.ds(tile * 256, 256)
            rhs = jnp.concatenate([gt_ref[pl.ds(start, 128), cols] for start in starts], 0)
            got = jnp.dot(lhs, rhs, preferred_element_type=F32)
            for n, row in enumerate(out_rows):
                where = pl.ds(pl.multiple_of(row + FIRST[k] * 16, 16), rows)
                out_ref[where, cols] += got[n * rows:(n + 1) * rows]

    if "z" in lows:
        @pl.loop(0, 2)
        def _(n):
            z = lows["z"] + n
            high = natural(z, "z") // 2
            pairs = [(y, x) for y in spots_of("y") for x in spots_of("x")]
            for first in range(0, len(pairs), 8):
                product([[(core, z, y, x) for y, x in pairs[first:first + 8]] for core in range(2)],
                        [(core * 2 + high) * 256 for core in range(2)])
        return

    @pl.loop(0, 2)
    def _(z_low):
        pairs = [(y, x) for y in spots_of("y") for x in spots_of("x")]
        blocks, out_rows = [], []
        for core in range(2):
            for high in range(2):
                z = spot(high * 2 + z_low, turned(k, "z"))
                blocks.append([(core, z, y, x) for y, x in pairs])
                out_rows.append((core * 2 + high) * 256)
        product(blocks, out_rows)


def kernel(
    act_hbm, og_hbm, pin_hbm, pout_hbm, ids_hbm, order_hbm, f_hbm, g_hbm, out_ref,
    ids_ref, order_ref, act, og, pin, pout, part, from_mate, mine, arrived, t0, t1, t2, t3, t4, t5, tok, fisher,
    counts_ref, their_counts, counts_sum, counts, dg, acc, lacc, q0, q1, q2, q3, q4, q5, g_ref, gt_ref,
    load_sem, mate_sem, rs_out, rs_in, f_out, f_in, f_pass, f_own, c_out, c_in, c_sem, g_sem, *sems):
    me = Place()
    bufs, qbufs = (t0, t1, t2, t3, t4, t5), (q0, q1, q2, q3, q4, q5)
    low, high, core = lax.rem(me.y, 2), me.y // 2, me.core
    p = low * 4 + me.x
    place = me.x * 2 + low

    def tp_mate(dx, dy):
        return lax.rem(me.x + dx, 4), lax.rem(low + dy, 2)

    def idx_mate(dz, dy):
        return me.device(z=lax.rem(me.z + dz, 4), y=lax.rem(high + dy, 2) * 2 + low)

    others = [me.device(x=x, y=high * 2 + y) for x, y in (tp_mate(*d) for d in OTHERS_TP)]
    far = [idx_mate(*d) for d in OTHERS_IDX]

    loads = [pltpu.make_async_copy(s, d, load_sem.at[n]) for n, (s, d) in enumerate(
        ((ids_hbm, ids_ref), (order_hbm, order_ref), (pin_hbm, pin), (act_hbm, act), (pout_hbm, pout), (og_hbm, og)))]
    for load in loads:
        load.start()

    def columns(x, y_low):
        block = lax.rem(me.z, 2) * 16 + (high * 2 + y_low) * 4 + x
        return f_hbm.at[:, pl.ds(pl.multiple_of(block * 128, 128), 128)]

    own_f = pltpu.make_async_copy(columns(me.x, low), fisher.at[place, core], f_own)
    own_f.start()
    friends = cell_mates(me) + others + far
    barrier = pltpu.get_barrier_semaphore()
    for device in friends:
        pl.semaphore_signal(barrier, inc=1, device_id=device, device_id_type=MESH)

    loads[0].wait()
    loads[1].wait()
    ids = jnp.concatenate([ids_ref[...]] * 16, 0).T
    less, same_doc = [0] * 8, [0] * 8
    for c in range(8):
        column = jnp.broadcast_to(ids[:, c:c + 1], (128, 128))
        for r in range(8):
            wanted = jnp.broadcast_to(order_ref[r:r + 1, :], (128, 128))
            below = jnp.where(column < wanted, 1, 0).reshape(16, 8, 128)
            equal = jnp.where(column == wanted, 1, 0).reshape(16, 8, 128)
            less[r] = less[r] + jnp.sum(below, 0)
            same_doc[r] = same_doc[r] + jnp.sum(equal, 0)
    for r in range(8):
        counts_ref[r:r + 1, :] = jnp.sum(less[r], 0, keepdims=True)
        counts_ref[8 + r:9 + r, :] = jnp.sum(same_doc[r], 0, keepdims=True)
    for load in loads[2:]:
        load.wait()
    def load_g(n):
        cols = pl.ds(n * 512, 512)
        return pltpu.make_async_copy(g_hbm.at[:, cols], g_ref.at[n % 2], g_sem.at[n % 2])

    load_g(0).start()
    load_g(1).start()

    @pl.loop(0, 4)
    def _(n):
        rows = pl.ds(pl.multiple_of(n * 256, 256), 256)
        both = jnp.concatenate([
            lax.dot_general(act[rows, :], pin[...], LANES, preferred_element_type=F32),
            lax.dot_general(og[rows, :], pout[...], LANES, preferred_element_type=F32)], 1)
        part[pl.ds(n * 2, 2)] = both.reshape(2, 2, 64, 128)

    pl.semaphore_wait(barrier, len(friends))

    shard = lax.axis_index("idx")
    count_copies = []
    for n, device in enumerate(far):
        copy = remote(counts_ref, their_counts.at[shard], c_out.at[n], c_in.at[n], device)
        copy.start()
        count_copies.append(copy)
    f_copies = []
    for n, d in enumerate(OTHERS_TP):
        f_copies.append(remote(columns(*tp_mate(*d)), fisher.at[place, core], f_out.at[n], f_in.at[n], others[n]))

    to_mate = remote(part.at[:, 1 - core], from_mate, mate_sem.at[0], mate_sem.at[1], me.mate())
    to_mate.start()
    to_mate.wait()
    rs_copies = []
    for q in range(8):
        mine[q] = part[q, core] + from_mate[q]
    arrived[p] = mine[p]
    for n, d in enumerate(OTHERS_TP):
        x, y = tp_mate(*d)
        copy = remote(mine.at[y * 4 + x], arrived.at[p], rs_out.at[n], rs_in.at[n], others[n])
        copy.start()
        rs_copies.append(copy)

    their_counts[shard] = counts_ref[...]
    for copy in count_copies:
        copy.wait_recv()
    summed = their_counts[0]
    for n in range(1, 8):
        summed = summed + their_counts[n]
    counts_sum[...] = summed
    to_scalar = pltpu.make_async_copy(counts_sum, counts, c_sem)
    to_scalar.start()
    to_scalar.wait()


    def turn(*chunks):
        for n in chunks:
            load_g(n).wait()

            @pl.loop(0, 4)
            def _(block):
                cols = pl.ds(pl.multiple_of(block * 128, 128), 128)
                gt_ref[pl.ds(pl.multiple_of(n * 512 + block * 128, 128), 128), :] = g_ref[n % 2, :, cols].T

            if n < 6:
                load_g(n + 2).start()

    turn(0, 1)
    for copy in rs_copies:
        copy.wait_recv()
    total = arrived[0]
    for q in range(1, 8):
        total = total + arrived[q]
    gather = Gather(me, bufs, sems[:4])
    for k in range(COLOURS):
        own = gather.at(k, (), ())
        row = T_FIRST[k] * 8
        bufs[k][(core, *own)] = total[row:row + T_UNITS[k] * 8].reshape(T_UNITS[k], 8, 128)
    gather.start()
    for n in EARLY_F:
        f_copies[n].start()
    turn(2, 3, 4)

    def spread(octet):
        for k in range(COLOURS):
            z0, y0, x0 = gather.cell(k, octet)
            zs, ys, xs = ([lax.rem(v + n + turned(k, a), 4) for n in range(2)]
                          for a, v in (("z", z0), ("y", y0), ("x", x0)))
            for n in range(8):
                a, b, c = n // 4, n // 2 % 2, n % 2
                chip = zs[a] * 16 + ys[b] * 4 + xs[c]
                for side in range(2):
                    base = pl.multiple_of(chip * 128 + side * 64 + T_FIRST[k] * 8, 8)
                    tok[pl.ds(base, T_UNITS[k] * 8), :] = bufs[k][side, z0 + a, y0 + b, x0 + c].reshape(
                        T_UNITS[k] * 8, 128)

    tok[8192:8224, :] = jnp.zeros((32, 128), F32)
    for n, octet in enumerate(OCTETS):
        gather.take(octet)
        if n == 0:
            turn(5, 6, 7)
        if n:
            gather.from_mate(OCTETS[n - 1])
            spread(OCTETS[n - 1])
        if n == 1:
            for m in LATE_F:
                f_copies[m].start()
        if n == 3:
            for m in LAST_F:
                f_copies[m].start()
    gather.from_mate(OCTETS[7])
    spread(OCTETS[7])

    first_row = (core * 2 + me.z // 2) * 256
    lane = lax.broadcasted_iota(jnp.int32, (128, 128), 1)
    sub = lax.broadcasted_iota(jnp.int32, (32, 128), 0)
    same = lax.broadcasted_iota(jnp.int32, (128, 256), 0) // 32 == lax.rem(
        lax.broadcasted_iota(jnp.int32, (128, 256), 1), 128) // 32

    def sum_tokens(group):
        rows = []
        for q in range(4):
            r = first_row + group * 4 + q
            start = counts[r // 128, lax.rem(r, 128)]
            length = counts[8 + r // 128, lax.rem(r, 128)]
            rows.append(jnp.where(sub < length, tok[pl.ds(start, 32), :], 0.0))
        pieces = jnp.concatenate(rows, 0)
        lead = pieces.T
        lead = jnp.concatenate([lead[64:96], lead[96:128]], 1)
        lead = jnp.where(same, jnp.concatenate([lead] * 4, 0), 0.0)
        lead_high, lead_low = halves(lead)
        top = jnp.where(lane < 64, pieces, 0.0)
        bottom = jnp.where(lane < 64, 0.0, pltpu.roll(pieces, 64, 1))
        right_high, right_low = halves(jnp.concatenate([top, bottom], 0))
        both = jnp.dot(lead_high, jnp.concatenate([right_high, right_low], 1), preferred_element_type=F32)
        rest = jnp.dot(lead_low, right_high, preferred_element_type=F32)
        got = both[:, :128] + both[:, 128:] + rest
        for q in range(4):
            dg[pl.ds(group * 4 + q, 32, stride=PITCH), :] = got[q * 32:(q + 1) * 32]

    pl.loop(0, 32, unroll=8)(sum_tokens)
    own_f.wait()
    for copy in f_copies:
        copy.wait_recv()
    pass_f = remote(fisher.at[:, core], fisher.at[:, core], f_pass.at[0], f_pass.at[1], me.mate())
    pass_f.start()
    pl.loop(32, 64, unroll=8)(sum_tokens)
    pass_f.wait_recv()
    acc[...] = jnp.zeros_like(acc)
    lacc[...] = jnp.zeros_like(lacc)

    @pl.loop(0, 16, unroll=4)
    def _(kk):
        left = dg[pl.ds(pl.multiple_of(kk * 2 * PITCH, 8), 256), :]
        right = dg[pl.ds(pl.multiple_of((kk * 2 + 1) * PITCH, 8), 256), :]
        d_high, d_low = halves(jnp.concatenate([left, right], 1))
        tiles = []
        for n in range(2):
            for half in range(2):
                lead = kk * 2 + n + half * 32
                tiles.append(fisher[lead // 8, lax.rem(lead // 4, 2), pl.ds(pl.multiple_of(
                    lax.rem(lead, 4) * 64, 64), 64), :])
        f_high, f_low = halves(jnp.concatenate(tiles, 0))
        acc[...] += jnp.dot(d_high, jnp.concatenate([f_high, f_low], 1), preferred_element_type=F32)
        lacc[...] += jnp.dot(d_low, f_high, preferred_element_type=F32)

    block = (acc[:, :128] + acc[:, 128:] + lacc[...]).astype(BF16)
    scores = Gather(me, qbufs, sems[4:])
    for k in range(COLOURS):
        first = FIRST[k] * 16
        qbufs[k][(core, *scores.at(k, (), ()))] = block[first:first + UNITS[k] * 16].reshape(UNITS[k], 16, 128)
    scores.start()
    out_ref[...] = jnp.zeros_like(out_ref)
    for octet in OCTETS[:4]:
        scores.take(octet)
    for octet in OCTETS[:4]:
        scores.from_mate(octet)
    for n, octet in enumerate(OCTETS[4:]):
        for k in range(2 * n, min(2 * n + 2, COLOURS)):
            multiply(scores, k, {5: 0}, qbufs, gt_ref, out_ref)
        if n < 3:
            scores.take(octet)
    for octet in OCTETS[4:6]:
        scores.from_mate(octet)
    for k in range(COLOURS):
        multiply(scores, k, {4: 0, 5: 1}, qbufs, gt_ref, out_ref)
        if k == 3:
            scores.take(OCTETS[7])
    for octet in OCTETS[6:]:
        scores.from_mate(octet)
    for k in range(COLOURS):
        multiply(scores, k, {4: 1, 5: 1}, qbufs, gt_ref, out_ref)

    for copy in count_copies + f_copies + rs_copies + [pass_f]:
        copy.wait_send()
    gather.close()
    scores.close()


EARLY_F = (0, 1, 5)
LATE_F = (2, 6)
LAST_F = (3, 4)


def per_device(activations, out_grads, proj_in, proj_out, doc_ids, doc_order, inv_fisher, index_grads):
    vmem, hbm = pl.BlockSpec(memory_space=pltpu.VMEM), pl.BlockSpec(memory_space=pltpu.HBM)
    dma = pltpu.SemaphoreType.DMA
    scratch = [pltpu.VMEM((8, 128), jnp.int32), pltpu.VMEM((8, 128), jnp.int32)]
    scratch += [pltpu.VMEM((1024, 1792), BF16), pltpu.VMEM((1024, 512), BF16), pltpu.VMEM((64, 1792), BF16),
               pltpu.VMEM((64, 512), BF16), pltpu.VMEM((8, 2, 64, 128), F32)]
    scratch += [pltpu.VMEM((8, 64, 128), F32)] * 3
    scratch += [pltpu.VMEM((2, 4, 4, 4, n, 8, 128), F32) for n in T_UNITS]
    scratch += [pltpu.VMEM((8224, 128), F32), pltpu.VMEM((8, 2, 256, 128), F32),
                pltpu.VMEM((16, 128), jnp.int32), pltpu.VMEM((8, 16, 128), jnp.int32),
                pltpu.VMEM((16, 128), jnp.int32), pltpu.SMEM((16, 128), jnp.int32),
                pltpu.VMEM((32 * PITCH, 128), F32), pltpu.VMEM((256, 256), F32), pltpu.VMEM((256, 128), F32)]
    scratch += [pltpu.VMEM((2, 4, 4, 4, n, 16, 128), BF16) for n in UNITS]
    scratch += [pltpu.VMEM((2, 1024, 512), BF16), pltpu.VMEM((4096, 1024), BF16)]
    scratch += [dma((6,)), dma((2,)), dma((7,)), dma((7,)), dma((7,)), dma((7,)), dma((2,)), dma, dma((7,)), dma((7,)),
                dma, dma((2,))]
    return pl.pallas_call(
        kernel,
        out_shape=pltpu.VMEM((1024, 1024), F32),
        in_specs=[hbm] * 8,
        out_specs=vmem,
        scratch_shapes=scratch + Gather.semaphores() + Gather.semaphores(),
        compiler_params=pltpu.CompilerParams(collective_id=2, has_side_effects=True, vmem_limit_bytes=46 << 20),
        name="influence",
    )(*(pltpu.with_memory_space_constraint(a, pltpu.HBM) for a in (
        activations, out_grads, proj_in.T, proj_out.T, doc_ids.reshape(8, 128), doc_order.reshape(8, 128),
        inv_fisher, index_grads)))


def solution(mesh):
    placed = (
        P("idx", "tp"), P("idx", "tp"), P("tp", None), P("tp", None),
        P("idx"), P(), P("tp", None), P(("idx", "tp"), None),
    )
    return jax.shard_map(
        per_device, mesh=mesh, in_specs=placed, out_specs=P(None, ("idx", "tp")), check_vma=False)
```

```python
import functools

import jax
import jax.numpy as jnp
from jax import lax
from jax.experimental import pallas as pl
from jax.experimental.pallas import tpu as pltpu
from jax.sharding import PartitionSpec as P

MESH = pl.DeviceIdType.MESH
F32, BF16 = jnp.float32, jnp.bfloat16
LINKS = (("x", 0), ("y", 0), ("z", 0), ("x", 1), ("y", 1), ("z", 1))
COLOURS = 6


class Place:
    def __init__(self):
        idx, tp = lax.axis_index("idx"), lax.axis_index("tp")
        self.x, self.z = tp // 4, idx // 2
        self.y = lax.rem(idx, 2) * 2 + lax.rem(tp // 2, 2)
        self.core = lax.rem(tp, 2)

    def device(self, x=None, y=None, z=None, core=None):
        x = self.x if x is None else x
        y = self.y if y is None else y
        z = self.z if z is None else z
        core = self.core if core is None else core
        return (z * 2 + y // 2, (x * 2 + lax.rem(y, 2)) * 2 + core)

    def across(self, axis, kind):
        v = getattr(self, axis)
        if kind:
            return lax.rem(v + 3 + 2 * lax.rem(v, 2), 4)
        return v + 1 - 2 * lax.rem(v, 2)

    def mate(self):
        return self.device(core=1 - self.core)

    def next_to(self, axis, kind):
        return self.device(**{axis: self.across(axis, kind)})


SUBSETS = [tuple(s for s in (0, 1, 2) if n >> s & 1) for n in (0, 1, 2, 4, 3, 5, 6, 7)]
OCTETS = [(), (3,), (4,), (3, 4), (5,), (3, 5), (4, 5), (3, 4, 5)]


def order_of(colour):
    return [LINKS[(colour + s) % 6] for s in range(6)]


def turned(colour, axis):
    order = order_of(colour)
    return 1 if order.index((axis, 1)) < order.index((axis, 0)) else 0


def spot(v, turn):
    return lax.rem(v + 3 * turn, 4)


class Gather:
    def __init__(self, me, bufs, sems, fine):
        self.me, self.bufs, self.fine = me, bufs, fine
        self.out_sem, self.in_sem, self.pass_in = sems
        self.places = {}
        for axis in "xyz":
            for turn in range(2):
                p = spot(getattr(me, axis), turn)
                over = lax.rem(p + 3 + 2 * lax.rem(p, 2), 4)
                for crossed, base in enumerate((p, over)):
                    self.places[axis, turn, 0, crossed] = base
                    self.places[axis, turn, 1, crossed] = base + 1 - 2 * lax.rem(base, 2)

    @staticmethod
    def semaphores(fine):
        dma = pltpu.SemaphoreType.DMA
        return [dma((COLOURS, 7)), dma((COLOURS, 24 if fine else 16)), dma((COLOURS, 8))]

    def at(self, k, subset, octet):
        order = order_of(k)
        got = []
        for axis in "zyx":
            flip = any(order[s][0] == axis for s in subset)
            crossed = any(order[s][0] == axis for s in octet)
            got.append(self.places[axis, turned(k, axis), int(flip), int(crossed)])
        return got

    def cell(self, k, octet):
        got = []
        for axis in "zyx":
            crossed = any(order_of(k)[s][0] == axis for s in octet)
            base = self.places[axis, turned(k, axis), 0, int(crossed)]
            got.append(base - lax.rem(base, 2))
        return got

    def cell_ref(self, k, core, octet):
        z, y, x = self.cell(k, octet)
        return self.bufs[k].at[core, pl.ds(z, 2), pl.ds(y, 2), pl.ds(x, 2)]

    def send(self, k, ref, out, into, device):
        return pltpu.make_async_remote_copy(
            src_ref=ref, dst_ref=ref, send_sem=self.out_sem.at[k, out], recv_sem=self.in_sem.at[k, into],
            device_id=device, device_id_type=MESH)

    def direct(self, k, n):
        move = {}
        for s in SUBSETS[n]:
            axis, kind = order_of(k)[s]
            move[axis] = self.me.across(axis, kind)
        ref = self.bufs[k].at[(self.me.core, *self.at(k, (), ()))]
        return self.send(k, ref, (0, 2, 1, 1, 3, 3, 3, 3)[n], n, self.me.device(**move))

    def onward(self, k, step, octet):
        axis, kind = order_of(k)[step]
        reached = OCTETS.index(octet + (step,))
        return self.send(k, self.cell_ref(k, self.me.core, octet), 1 + step, 8 + reached,
                         self.me.next_to(axis, kind))

    def single(self, k, n):
        ref = self.bufs[k].at[(self.me.core, *self.at(k, SUBSETS[n], ()))]
        return self.send(k, ref, 4, 16 + n, self.me.next_to(*order_of(k)[3]))

    def arrive(self, k, octet):
        if octet == (3,) and self.fine:
            for n in range(8):
                ref = self.bufs[k].at[(self.me.core, *self.at(k, SUBSETS[n], octet))]
                self.send(k, ref, 0, 16 + n, self.me.mate()).wait_recv()
            return
        ref = self.cell_ref(k, self.me.core, octet)
        self.send(k, ref, 0, 8 + OCTETS.index(octet), self.me.mate()).wait_recv()

    def passed(self, k, octet, core):
        n = OCTETS.index(octet)
        ref = self.cell_ref(k, core, octet)
        return pltpu.make_async_remote_copy(
            src_ref=ref, dst_ref=ref, send_sem=self.out_sem.at[k, 0], recv_sem=self.pass_in.at[k, n],
            device_id=self.me.mate(), device_id_type=MESH)

    def start(self):
        for n in (7, 4, 5, 6, 1, 2, 3):
            for k in range(COLOURS):
                self.direct(k, n).start()
        if self.fine:
            for k in range(COLOURS):
                self.single(k, 0).start()

    def forward(self, step, octet):
        for k in range(COLOURS):
            self.onward(k, step, octet).start()

    def take(self, octet):
        step = max((2,) + octet) + 1
        for n in range(1, 8):
            for k in range(COLOURS):
                if octet == ():
                    ref = self.bufs[k].at[(self.me.core, *self.at(k, SUBSETS[n], ()))]
                    self.send(k, ref, 0, n, self.me.mate()).wait_recv()
                    if self.fine:
                        self.single(k, n).start()
        if octet == ():
            if not self.fine:
                self.forward(3, ())
            self.forward(4, ())
        for k in range(COLOURS):
            if octet:
                self.arrive(k, octet)
            if octet and step < 6:
                self.onward(k, step, octet).start()
        if octet == (3,):
            self.forward(5, ())
            self.forward(5, (3,))
        for k in range(COLOURS):
            self.passed(k, octet, self.me.core).start()

    def from_mate(self, octet):
        for k in range(COLOURS):
            self.passed(k, octet, 1 - self.me.core).wait_recv()

    def close(self):
        for k in range(COLOURS):
            whole = self.bufs[k].at[0]
            for n, ref in enumerate((
                    whole, whole.at[0, 0, pl.ds(0, 2)], whole.at[0, 0, 0], whole.at[0, 0],
                    whole.at[0, pl.ds(0, 2)], whole.at[0], whole.at[pl.ds(0, 2)])):
                self.send(k, ref, n, 0, self.me.mate()).wait_send()


def cell_mates(me):
    found = {}
    for k in range(COLOURS):
        for subset in SUBSETS[1:]:
            steps = tuple(sorted(order_of(k)[n] for n in subset))
            found[steps] = me.device(**{axis: me.across(axis, kind) for axis, kind in steps})
    return list(found.values()) + [me.mate()]


def remote(src, dst, s, r, device):
    return pltpu.make_async_remote_copy(
        src_ref=src, dst_ref=dst, send_sem=s, recv_sem=r, device_id=device, device_id_type=MESH)


def halves(v):
    high = v.astype(BF16)
    return high, (v - high.astype(F32)).astype(BF16)


UNITS = (3, 3, 3, 3, 2, 2)
FIRST = (0, 3, 6, 9, 12, 14)
T_UNITS = (2, 1, 1, 2, 1, 1)
T_FIRST = (0, 2, 3, 4, 6, 7)
OTHERS_TP = [(dx, dy) for dx in range(4) for dy in range(2)][1:]
OTHERS_IDX = [(dz, dy) for dz in range(4) for dy in range(2)][1:]
PITCH = 264
LANES = (((1,), (1,)), ((), ()))


def multiply(gather, k, crossed, bufs, gt_ref, out_ref):
    rows = UNITS[k] * 16
    lows = {}
    for step, over in crossed.items():
        axis = order_of(k)[step][0]
        low = gather.places[axis, turned(k, axis), 0, over]
        lows[axis] = low - lax.rem(low, 2)

    def spots_of(axis):
        return [lows[axis] + n for n in range(2)] if axis in lows else list(range(4))

    def natural(p, a):
        return lax.rem(p + turned(k, a), 4)

    def product(spots, out_rows):
        starts = []
        for _, z, y, x in spots[0]:
            zn, yn, xn = natural(z, "z"), natural(y, "y"), natural(x, "x")
            starts.append(pl.multiple_of((zn // 2 * 16 + yn * 4 + xn) * 128, 128))
        lhs = jnp.concatenate([
            jnp.concatenate([bufs[k][s].reshape(rows, 128) for s in blocks], 1) for blocks in spots], 0)
        for tile in range(4):
            cols = pl.ds(tile * 256, 256)
            rhs = jnp.concatenate([gt_ref[pl.ds(start, 128), cols] for start in starts], 0)
            got = jnp.dot(lhs, rhs, preferred_element_type=F32)
            for n, row in enumerate(out_rows):
                where = pl.ds(pl.multiple_of(row + FIRST[k] * 16, 16), rows)
                out_ref[where, cols] += got[n * rows:(n + 1) * rows]

    pairs = [(y, x) for y in spots_of("y") for x in spots_of("x")]

    def whole(z_high):
        for first in range(0, len(pairs), 8):
            blocks, out_rows = [], []
            for core in range(2):
                for z_low in range(2):
                    z = spot(z_high * 2 + z_low, turned(k, "z"))
                    blocks.append([(core, z, y, x) for y, x in pairs[first:first + 8]])
                    out_rows.append((core * 2 + z_low) * 256)
            product(blocks, out_rows)

    if "z" in lows and not turned(k, "z"):
        whole(lows["z"] // 2)
        return

    @pl.loop(0, 2)
    def _(n):
        if "z" not in lows:
            whole(n)
            return
        z = lows["z"] + n
        z_low = lax.rem(natural(z, "z"), 2)
        for first in range(0, len(pairs), 8):
            product([[(core, z, y, x) for y, x in pairs[first:first + 8]] for core in range(2)],
                    [(core * 2 + z_low) * 256 for core in range(2)])


def kernel(
    act_hbm, og_hbm, pin_hbm, pout_hbm, ids_hbm, order_hbm, f_hbm, g_hbm, out_ref,
    ids_ref, order_ref, act, og, pin, pout, part, from_mate, mine, arrived, t0, t1, t2, t3, t4, t5, tok, fisher,
    counts_ref, their_counts, counts_sum, counts, dg, acc, lacc, q0, q1, q2, q3, q4, q5, g_ref, gt_ref,
    load_sem, mate_sem, rs_out, rs_in, f_out, f_in, f_pass, f_own, c_out, c_in, c_sem, g_sem, *sems):
    me = Place()
    bufs, qbufs = (t0, t1, t2, t3, t4, t5), (q0, q1, q2, q3, q4, q5)
    low, high, core = lax.rem(me.y, 2), me.y // 2, me.core
    p = low * 4 + me.x
    place = me.x * 2 + low

    def tp_mate(dx, dy):
        return lax.rem(me.x + dx, 4), lax.rem(low + dy, 2)

    def idx_mate(dz, dy):
        return me.device(z=lax.rem(me.z + dz, 4), y=lax.rem(high + dy, 2) * 2 + low)

    others = [me.device(x=x, y=high * 2 + y) for x, y in (tp_mate(*d) for d in OTHERS_TP)]
    far = [idx_mate(*d) for d in OTHERS_IDX]

    loads = [pltpu.make_async_copy(s, d, load_sem.at[n]) for n, (s, d) in enumerate(
        ((ids_hbm, ids_ref), (order_hbm, order_ref), (pin_hbm, pin), (pout_hbm, pout), (og_hbm, og))
        + tuple((act_hbm.at[rows], act.at[rows]) for rows in (pl.ds(n * 256, 256) for n in range(4))))]
    for load in loads:
        load.start()

    def columns(x, y_low):
        block = me.z // 2 * 16 + (high * 2 + y_low) * 4 + x
        return f_hbm.at[:, pl.ds(pl.multiple_of(block * 128, 128), 128)]

    own_f = pltpu.make_async_copy(columns(me.x, low), fisher.at[place, core], f_own)
    own_f.start()
    friends = cell_mates(me) + others + far
    barrier = pltpu.get_barrier_semaphore()
    for device in friends:
        pl.semaphore_signal(barrier, inc=1, device_id=device, device_id_type=MESH)

    for load in loads[2:5]:
        load.wait()
    def load_g(n):
        cols = pl.ds(n * 512, 512)
        return pltpu.make_async_copy(g_hbm.at[:, cols], g_ref.at[n % 2], g_sem.at[n % 2])

    load_g(0).start()
    load_g(1).start()

    for n in range(4):
        loads[5 + n].wait()
        rows = pl.ds(n * 256, 256)
        both = jnp.concatenate([
            lax.dot_general(act[rows, :], pin[...], LANES, preferred_element_type=F32),
            lax.dot_general(og[rows, :], pout[...], LANES, preferred_element_type=F32)], 1)
        part[pl.ds(n * 2, 2)] = both.reshape(2, 2, 64, 128)

    pl.semaphore_wait(barrier, len(friends))

    f_copies = []
    for n, d in enumerate(OTHERS_TP):
        f_copies.append(remote(columns(*tp_mate(*d)), fisher.at[place, core], f_out.at[n], f_in.at[n], others[n]))

    for n in EARLY_F:
        f_copies[n].start()
    to_mate = remote(part.at[:, 1 - core], from_mate, mate_sem.at[0], mate_sem.at[1], me.mate())
    to_mate.start()
    to_mate.wait()
    rs_copies = []
    for q in range(8):
        mine[q] = part[q, core] + from_mate[q]
    arrived[p] = mine[p]
    for n, d in enumerate(OTHERS_TP):
        x, y = tp_mate(*d)
        copy = remote(mine.at[y * 4 + x], arrived.at[p], rs_out.at[n], rs_in.at[n], others[n])
        copy.start()
        rs_copies.append(copy)

    loads[0].wait()
    loads[1].wait()
    ids = jnp.concatenate([ids_ref[...]] * 16, 0).T
    less, same_doc = [0] * 8, [0] * 8
    for c in range(8):
        column = jnp.broadcast_to(ids[:, c:c + 1], (128, 128))
        for r in range(8):
            wanted = jnp.broadcast_to(order_ref[r:r + 1, :], (128, 128))
            below = jnp.where(column < wanted, 1, 0).reshape(16, 8, 128)
            equal = jnp.where(column == wanted, 1, 0).reshape(16, 8, 128)
            less[r] = less[r] + jnp.sum(below, 0)
            same_doc[r] = same_doc[r] + jnp.sum(equal, 0)
    for r in range(8):
        counts_ref[r:r + 1, :] = jnp.sum(less[r], 0, keepdims=True)
        counts_ref[8 + r:9 + r, :] = jnp.sum(same_doc[r], 0, keepdims=True)
    shard = lax.axis_index("idx")
    count_copies = []
    for n, device in enumerate(far):
        copy = remote(counts_ref, their_counts.at[shard], c_out.at[n], c_in.at[n], device)
        copy.start()
        count_copies.append(copy)
    their_counts[shard] = counts_ref[...]

    def turn(*chunks):
        for n in chunks:
            load_g(n).wait()

            @pl.loop(0, 4)
            def _(block):
                cols = pl.ds(pl.multiple_of(block * 128, 128), 128)
                gt_ref[pl.ds(pl.multiple_of(n * 512 + block * 128, 128), 128), :] = g_ref[n % 2, :, cols].T

            if n < 6:
                load_g(n + 2).start()

    turn(0, 1)
    for copy in rs_copies:
        copy.wait_recv()
    total = arrived[0]
    for q in range(1, 8):
        total = total + arrived[q]
    gather = Gather(me, bufs, sems[:3], False)
    for k in range(COLOURS):
        own = gather.at(k, (), ())
        row = T_FIRST[k] * 8
        bufs[k][(core, *own)] = total[row:row + T_UNITS[k] * 8].reshape(T_UNITS[k], 8, 128)
    gather.start()
    for n in LATE_F:
        f_copies[n].start()
    turn(2, 3, 4)

    def spread(octet):
        for k in range(COLOURS):
            z0, y0, x0 = gather.cell(k, octet)
            zs, ys, xs = ([lax.rem(v + n + turned(k, a), 4) for n in range(2)]
                          for a, v in (("z", z0), ("y", y0), ("x", x0)))
            for n in range(8):
                a, b, c = n // 4, n // 2 % 2, n % 2
                chip = zs[a] * 16 + ys[b] * 4 + xs[c]
                for side in range(2):
                    base = pl.multiple_of(chip * 128 + side * 64 + T_FIRST[k] * 8, 8)
                    tok[pl.ds(base, T_UNITS[k] * 8), :] = bufs[k][side, z0 + a, y0 + b, x0 + c].reshape(
                        T_UNITS[k] * 8, 128)

    tok[8192:8224, :] = jnp.zeros((32, 128), F32)
    for n, octet in enumerate(OCTETS):
        gather.take(octet)
        if n == 0:
            turn(5, 6, 7)
        if n:
            gather.from_mate(OCTETS[n - 1])
            spread(OCTETS[n - 1])
        if n == 1:
            for copy in count_copies:
                copy.wait_recv()
            summed = their_counts[0]
            for n in range(1, 8):
                summed = summed + their_counts[n]
            counts_sum[...] = summed
            to_scalar = pltpu.make_async_copy(counts_sum, counts, c_sem)
            to_scalar.start()
        if n == 3:
            for m in LAST_F:
                f_copies[m].start()
    gather.from_mate(OCTETS[7])
    spread(OCTETS[7])

    to_scalar.wait()
    first_row = (core * 2 + lax.rem(me.z, 2)) * 256
    lane = lax.broadcasted_iota(jnp.int32, (128, 128), 1)
    sub = lax.broadcasted_iota(jnp.int32, (32, 128), 0)
    same = lax.broadcasted_iota(jnp.int32, (128, 256), 0) // 32 == lax.rem(
        lax.broadcasted_iota(jnp.int32, (128, 256), 1), 128) // 32

    def sum_tokens(group):
        rows = []
        for q in range(4):
            r = first_row + group * 4 + q
            start = counts[r // 128, lax.rem(r, 128)]
            length = counts[8 + r // 128, lax.rem(r, 128)]
            rows.append(jnp.where(sub < length, tok[pl.ds(start, 32), :], 0.0))
        pieces = jnp.concatenate(rows, 0)
        lead = pieces.T
        lead = jnp.concatenate([lead[64:96], lead[96:128]], 1)
        lead = jnp.where(same, jnp.concatenate([lead] * 4, 0), 0.0)
        lead_high, lead_low = halves(lead)
        top = jnp.where(lane < 64, pieces, 0.0)
        bottom = jnp.where(lane < 64, 0.0, pltpu.roll(pieces, 64, 1))
        right_high, right_low = halves(jnp.concatenate([top, bottom], 0))
        both = jnp.dot(lead_high, jnp.concatenate([right_high, right_low], 1), preferred_element_type=F32)
        rest = jnp.dot(lead_low, right_high, preferred_element_type=F32)
        got = both[:, :128] + both[:, 128:] + rest
        for q in range(4):
            dg[pl.ds(group * 4 + q, 32, stride=PITCH), :] = got[q * 32:(q + 1) * 32]

    pl.loop(0, 32, unroll=8)(sum_tokens)
    own_f.wait()
    for copy in f_copies:
        copy.wait_recv()
    pass_f = remote(fisher.at[:, core], fisher.at[:, core], f_pass.at[0], f_pass.at[1], me.mate())
    pass_f.start()
    pl.loop(32, 64, unroll=8)(sum_tokens)
    pass_f.wait_recv()
    acc[...] = jnp.zeros_like(acc)
    lacc[...] = jnp.zeros_like(lacc)

    @pl.loop(0, 16, unroll=4)
    def _(kk):
        left = dg[pl.ds(pl.multiple_of(kk * 2 * PITCH, 8), 256), :]
        right = dg[pl.ds(pl.multiple_of((kk * 2 + 1) * PITCH, 8), 256), :]
        d_high, d_low = halves(jnp.concatenate([left, right], 1))
        tiles = []
        for n in range(2):
            for half in range(2):
                lead = kk * 2 + n + half * 32
                tiles.append(fisher[lead // 8, lax.rem(lead // 4, 2), pl.ds(pl.multiple_of(
                    lax.rem(lead, 4) * 64, 64), 64), :])
        f_high, f_low = halves(jnp.concatenate(tiles, 0))
        acc[...] += jnp.dot(d_high, jnp.concatenate([f_high, f_low], 1), preferred_element_type=F32)
        lacc[...] += jnp.dot(d_low, f_high, preferred_element_type=F32)

    block = (acc[:, :128] + acc[:, 128:] + lacc[...]).astype(BF16)
    scores = Gather(me, qbufs, sems[3:], True)
    for k in range(COLOURS):
        first = FIRST[k] * 16
        qbufs[k][(core, *scores.at(k, (), ()))] = block[first:first + UNITS[k] * 16].reshape(UNITS[k], 16, 128)
    scores.start()
    out_ref[...] = jnp.zeros_like(out_ref)
    scores.take(OCTETS[0])
    scores.from_mate(OCTETS[0])
    for k in range(COLOURS):
        multiply(scores, k, {3: 0, 4: 0, 5: 0}, qbufs, gt_ref, out_ref)
    scores.take(OCTETS[1])
    scores.from_mate(OCTETS[1])

    def part_scores(crossed, meanwhile):
        for k in range(COLOURS):
            multiply(scores, k, crossed, qbufs, gt_ref, out_ref)
            if k in meanwhile:
                scores.take(OCTETS[meanwhile[k]])

    part_scores({3: 1, 4: 0, 5: 0}, {2: 2, 5: 3})
    scores.from_mate(OCTETS[2])
    scores.from_mate(OCTETS[3])
    part_scores({4: 1, 5: 0}, {1: 4, 4: 5})
    scores.from_mate(OCTETS[4])
    scores.from_mate(OCTETS[5])
    part_scores({4: 0, 5: 1}, {1: 6, 4: 7})
    scores.from_mate(OCTETS[6])
    scores.from_mate(OCTETS[7])
    part_scores({4: 1, 5: 1}, {})

    for copy in count_copies + f_copies + rs_copies + [pass_f]:
        copy.wait_send()
    gather.close()
    scores.close()


EARLY_F = (0, 1, 5)
LATE_F = (2, 6)
LAST_F = (3, 4)


def per_device(activations, out_grads, proj_in, proj_out, doc_ids, doc_order, inv_fisher, index_grads):
    vmem, hbm = pl.BlockSpec(memory_space=pltpu.VMEM), pl.BlockSpec(memory_space=pltpu.HBM)
    dma = pltpu.SemaphoreType.DMA
    scratch = [pltpu.VMEM((8, 128), jnp.int32), pltpu.VMEM((8, 128), jnp.int32)]
    scratch += [pltpu.VMEM((1024, 1792), BF16), pltpu.VMEM((1024, 512), BF16), pltpu.VMEM((64, 1792), BF16),
               pltpu.VMEM((64, 512), BF16), pltpu.VMEM((8, 2, 64, 128), F32)]
    scratch += [pltpu.VMEM((8, 64, 128), F32)] * 3
    scratch += [pltpu.VMEM((2, 4, 4, 4, n, 8, 128), F32) for n in T_UNITS]
    scratch += [pltpu.VMEM((8224, 128), F32), pltpu.VMEM((8, 2, 256, 128), F32),
                pltpu.VMEM((16, 128), jnp.int32), pltpu.VMEM((8, 16, 128), jnp.int32),
                pltpu.VMEM((16, 128), jnp.int32), pltpu.SMEM((16, 128), jnp.int32),
                pltpu.VMEM((32 * PITCH, 128), F32), pltpu.VMEM((256, 256), F32), pltpu.VMEM((256, 128), F32)]
    scratch += [pltpu.VMEM((2, 4, 4, 4, n, 16, 128), BF16) for n in UNITS]
    scratch += [pltpu.VMEM((2, 1024, 512), BF16), pltpu.VMEM((4096, 1024), BF16)]
    scratch += [dma((9,)), dma((2,)), dma((7,)), dma((7,)), dma((7,)), dma((7,)), dma((2,)), dma, dma((7,)), dma((7,)),
                dma, dma((2,))]
    return pl.pallas_call(
        kernel,
        out_shape=pltpu.VMEM((1024, 1024), F32),
        in_specs=[hbm] * 8,
        out_specs=vmem,
        scratch_shapes=scratch + Gather.semaphores(False) + Gather.semaphores(True),
        compiler_params=pltpu.CompilerParams(collective_id=2, has_side_effects=True, vmem_limit_bytes=46 << 20),
        name="influence",
    )(*(pltpu.with_memory_space_constraint(a, pltpu.HBM) for a in (
        activations, out_grads, proj_in.T, proj_out.T, doc_ids.reshape(8, 128), doc_order.reshape(8, 128),
        inv_fisher, index_grads)))


def solution(mesh):
    placed = (
        P("idx", "tp"), P("idx", "tp"), P("tp", None), P("tp", None),
        P("idx"), P(), P("tp", None), P(("idx", "tp"), None),
    )
    return jax.shard_map(
        per_device, mesh=mesh, in_specs=placed, out_specs=P(None, ("idx", "tp")), check_vma=False)
```
